32 devices in a mesh: clip: 2 (over y), seq: 4 (over z), head: 4 (over x, core).
Axes of the slice: x: 2, y: 2, z: 4, core: 2. Of those that a mesh axis runs over, the one named last changes fastest.
Arguments:
- queries: bfloat16 [16, 4, 16, 3072], P(('clip', 'head'), 'seq'), parts along dimension 0, may hold values from -15 to 15
- attn_keys: bfloat16 [16, 4, 16, 3072], P(('clip', 'head'), 'seq'), parts along dimension 0, may hold values from -5 to 5
- attn_values: bfloat16 [16, 4, 16, 3072], P(('clip', 'head'), 'seq'), parts along dimension 0, may hold values from -5 to 5
- residual: bfloat16 [16, 4, 16, 5120], P(('clip', 'head'), 'seq'), parts along dimension 0, may hold values from -6 to 6
- out_weight: bfloat16 [3072, 5120], P('head', 'seq'), may hold values from -0.109375 to 0.109375
- out_gate: float32 [5120], replicated, may hold values from 0.3 to 3
- head_shift: float32 [5120], replicated, may hold values from -3 to 3
- head_scale: float32 [5120], replicated, may hold values from -1.5 to 1.5
- head_weight: bfloat16 [5120, 64], replicated, may hold values from -0.078125 to 0.078125
- head_bias: float32 [64], replicated, may hold values from -3 to 3
- conv_weight: bfloat16 [3, 3, 3, 16, 384], replicated, may hold values from -0.3125 to 0.3125
- conv_bias: float32 [384], replicated, may hold values from -3 to 3
- norm_gain: float32 [384], replicated, may hold values from 0.5 to 2
Outputs:
- hidden: bfloat16 [16, 4, 16, 5120], P(('clip', 'head'), 'seq'), parts along dimension 0
- features: bfloat16 [16, 8, 32, 384], P(('clip', 'head'), 'seq'), parts along dimension 0
The draws below stay inside these ranges and needn't reach their ends.
There are 2 independent parts, one for each index of `clip`. The reference program is written for one: setup_inputs(seed, part) draws one part's arguments, and reference() takes and returns one part's arrays. A program takes and returns all parts, laid end to end along the dimension named above; an argument that names none is the same for every part. Nothing has to cross between parts.
All inputs are finite; a program needn't handle non-finite values.
Results may differ from the reference program's by a relative error of at most 0.013.
Values may be sent and summed in bfloat16 or wider, within the bound.
A program may use at most 128 MiB of HBM per device.

```python
import math
import jax
import jax.numpy as jnp
from jax import lax

D = 5120
HEAD_DIM = 128
HEADS = 24
LAT_CH = 16
VAE_CH = 384
WP = 16
F = 8
HP = 4
N_HEAD = 4


def draw_queries(key, part):
    count = F * HP * WP
    values = 3.0 * jnp.clip(jax.random.normal(jax.random.fold_in(key, 11), (count, HEADS, HEAD_DIM), jnp.float32), -5.0, 5.0)
    return values.reshape(F, HP, WP, HEADS * HEAD_DIM).astype(jnp.bfloat16)


def draw_attn_keys(key, part):
    count = F * HP * WP
    values = jnp.clip(jax.random.normal(jax.random.fold_in(key, 12), (count, HEADS, HEAD_DIM), jnp.float32), -5.0, 5.0)
    return values.reshape(F, HP, WP, HEADS * HEAD_DIM).astype(jnp.bfloat16)


def block_levels(own_key, dims, shards, low, top_value):
    def one(dim, shards_of):
        heights = jax.random.uniform(jax.random.fold_in(jax.random.fold_in(own_key, 6), dim), (shards_of,), jnp.float32, low / len(shards), top_value / len(shards))
        return jnp.repeat(jnp.exp(heights), dims[dim] // shards_of).reshape((-1,) + (1,) * (len(dims) - dim - 1))

    loudness = one(*shards[0])
    for cut in shards[1:]:
        loudness = loudness * one(*cut)
    return loudness


def centred(own_key, shape, deviation, reach, split=(), held_as=jnp.bfloat16):
    level = block_levels(own_key, shape, split, -0.22, 0.18) if split else 1.0
    entries = jax.random.normal(own_key, shape, jnp.float32) * deviation * level
    return jnp.minimum(jnp.maximum(entries, -reach), reach).astype(held_as)


def setup_inputs(seed: int = 0, part: int = 0) -> dict:
    key_list = jax.random.split(jax.random.key(seed), 14)
    own_keys = jax.random.split(jax.random.fold_in(key_list[13], part), 14)
    queries = draw_queries(jax.random.fold_in(jax.random.fold_in(key_list[13], part), 71), part)
    attn_keys = draw_attn_keys(jax.random.fold_in(jax.random.fold_in(key_list[13], part), 71), part)
    attn_values = centred(own_keys[2], (F, HP, WP, HEADS * HEAD_DIM), 1.0, 5.0, ((0, 4), (1, 4)))
    residual = centred(own_keys[3], (F, HP, WP, D), 1.0, 6.0, ((0, 4), (1, 4)))
    out_weight = centred(key_list[4], (HEADS * HEAD_DIM, D), (HEADS * HEAD_DIM) ** -0.5, 0.109375, ((0, 4), (1, 4)))
    out_gate = jnp.clip(jnp.exp(jax.random.uniform(key_list[5], (D,), jnp.float32, math.log(0.3), math.log(3.0))), 0.3, 3.0)
    head_shift = centred(key_list[6], (D,), 0.5, 3.0, (), jnp.float32)
    head_scale = centred(key_list[7], (D,), 0.3, 1.5, (), jnp.float32)
    head_weight = centred(key_list[8], (D, 4 * LAT_CH), D ** -0.5, 0.078125)
    head_bias = centred(key_list[9], (4 * LAT_CH,), 0.5, 3.0, (), jnp.float32)
    conv_weight = centred(key_list[10], (3, 3, 3, LAT_CH, VAE_CH), (27 * LAT_CH) ** -0.5, 0.3125)
    conv_bias = centred(key_list[11], (VAE_CH,), 0.5, 3.0, (), jnp.float32)
    norm_gain = jnp.clip(jnp.exp(jax.random.uniform(key_list[12], (VAE_CH,), jnp.float32, math.log(0.5), math.log(2.0))), 0.5, 2.0)
    return {"queries": queries, "attn_keys": attn_keys, "attn_values": attn_values, "residual": residual, "out_weight": out_weight, "out_gate": out_gate, "head_shift": head_shift, "head_scale": head_scale, "head_weight": head_weight, "head_bias": head_bias, "conv_weight": conv_weight, "conv_bias": conv_bias, "norm_gain": norm_gain}


def head_latent(hidden, head_shift, head_scale, head_weight, head_bias):
    values = hidden.astype(jnp.float32)
    center = values - lax.optimization_barrier(jnp.mean(values, -1, keepdims=True))
    spread = lax.optimization_barrier(jnp.mean(center * center, -1, keepdims=True))
    normed = (center * lax.rsqrt(spread + 1e-06) * (1.0 + head_scale) + head_shift).astype(jnp.bfloat16)
    flat = normed.reshape(-1, normed.shape[-1])
    latent = (jnp.dot(flat, head_weight, preferred_element_type=jnp.float32) + head_bias).astype(jnp.bfloat16)
    frames, height, breadth = (hidden.shape[0], hidden.shape[1], hidden.shape[2])
    channels = head_weight.shape[1] // 4
    patches = latent.reshape(frames, height, breadth, 2, 2, channels).transpose(0, 1, 3, 2, 4, 5)
    return patches.reshape(frames, height * 2, breadth * 2, channels)

def convolve(padded, frames, conv_weight, conv_bias, norm_gain):
    height = padded.shape[1] - 2
    breadth = padded.shape[2] - 2
    stacked = jnp.concatenate([padded[time_off:time_off + frames, row_off:row_off + height, col_off:col_off + breadth] for time_off in range(3) for row_off in range(3) for col_off in range(3)], -1)
    kernel = conv_weight.reshape(-1, conv_weight.shape[-1])
    linear = jnp.dot(stacked.reshape(-1, stacked.shape[-1]), kernel, preferred_element_type=jnp.float32) + conv_bias
    normed = linear * lax.rsqrt(lax.optimization_barrier(jnp.mean(linear * linear, -1, keepdims=True)) + 1e-06) * norm_gain
    return jax.nn.silu(normed).astype(jnp.bfloat16).reshape(frames, height, breadth, -1)

def one_head(triple):
    query_one, key_one, value_one = triple
    scores = jnp.dot(query_one, key_one.T, preferred_element_type=jnp.float32) * query_one.shape[-1] ** (-0.5)
    peak = lax.optimization_barrier(jnp.max(scores, -1, keepdims=True))
    weights = jnp.exp(scores - peak)
    denominator = lax.optimization_barrier(jnp.sum(weights, -1, keepdims=True))
    product = jnp.dot(weights.astype(jnp.bfloat16), value_one, preferred_element_type=jnp.float32)
    return (product / denominator).astype(jnp.bfloat16)

def add_group(running_sum, pair):
    term = jnp.dot(pair[0], pair[1], preferred_element_type=jnp.float32).astype(jnp.bfloat16)
    term = lax.optimization_barrier(term).astype(jnp.float32)
    return (running_sum + term, None)

def reference(queries, attn_keys, attn_values, residual, out_weight, out_gate, head_shift, head_scale, head_weight, head_bias, conv_weight, conv_bias, norm_gain):
    count = F * HP * WP
    query_heads = queries.reshape(count, HEADS, HEAD_DIM).transpose(1, 0, 2)
    key_heads = attn_keys.reshape(count, HEADS, HEAD_DIM).transpose(1, 0, 2)
    value_heads = attn_values.reshape(count, HEADS, HEAD_DIM).transpose(1, 0, 2)
    attended = lax.map(one_head, (query_heads, key_heads, value_heads))
    attended = attended.transpose(1, 0, 2).reshape(count, HEADS * HEAD_DIM)
    group_width = HEADS // N_HEAD * HEAD_DIM
    groups_in = attended.reshape(count, N_HEAD, group_width).transpose(1, 0, 2)
    weights_in = out_weight.reshape(N_HEAD, group_width, D)
    projected, _ = lax.scan(add_group, jnp.zeros((count, D), jnp.float32), (groups_in, weights_in))
    projected = projected.reshape(F, HP, WP, D)
    hidden = (residual.astype(jnp.float32) + out_gate * projected).astype(jnp.bfloat16)
    video = head_latent(hidden, head_shift, head_scale, head_weight, head_bias)
    padded = jnp.pad(video, ((2, 0), (1, 1), (1, 1), (0, 0)))
    features = convolve(padded, F, conv_weight, conv_bias, norm_gain)
    return (hidden, features)
```

```python
import functools
import math

import jax
import jax.numpy as jnp
from jax import lax
from jax.experimental import pallas as pl
from jax.experimental.pallas import tpu as pltpu
from jax.sharding import PartitionSpec as P

HEAD_DIM = 128


def from_behind(value, axis, steps):
    count = lax.axis_size(axis)
    first, last = (max(0, -steps), min(count, count - steps))
    return lax.ppermute(value, axis, [(source, source + steps) for source in range(first, last)])


def padded_2(x, sides, width):
    for axis, dim in sides:
        peers, length = (lax.axis_size(axis), x.shape[dim])
        up = [(i, (i + 1) % peers) for i in range(peers - 1)]
        down = [(j, i) for i, j in up]
        last = lax.slice_in_dim(x, length - width, length, axis=dim)
        first = lax.slice_in_dim(x, 0, width, axis=dim)
        before = lax.ppermute(last, axis, up)
        after = lax.ppermute(first, axis, down)
        x = jnp.concatenate([before, x, after], axis=dim)
    return x


def head_latent(hidden, head_shift, head_scale, head_weight, head_bias):
    values = hidden.astype(jnp.float32)
    center = values - jnp.mean(values, -1, keepdims=True)
    spread = jnp.mean(center * center, -1, keepdims=True)
    normed = (center * lax.rsqrt(spread + 1e-06) * (1.0 + head_scale) + head_shift).astype(
        jnp.bfloat16
    )
    flat = normed.reshape(-1, normed.shape[-1])
    latent = (jnp.dot(flat, head_weight, preferred_element_type=jnp.float32) + head_bias).astype(
        jnp.bfloat16
    )
    frames, height, breadth = (hidden.shape[0], hidden.shape[1], hidden.shape[2])
    channels = head_weight.shape[1] // 4
    patches = latent.reshape(frames, height, breadth, 2, 2, channels).transpose(0, 1, 3, 2, 4, 5)
    return patches.reshape(frames, height * 2, breadth * 2, channels)


def convolve(padded, frames, conv_weight, conv_bias, norm_gain):
    height = padded.shape[1] - 2
    breadth = padded.shape[2] - 2
    stacked = jnp.concatenate(
        [
            padded[
                time_off : time_off + frames,
                row_off : row_off + height,
                col_off : col_off + breadth,
            ]
            for time_off in range(3)
            for row_off in range(3)
            for col_off in range(3)
        ],
        -1,
    )
    kernel = conv_weight.reshape(-1, conv_weight.shape[-1])
    linear = (
        jnp.dot(stacked.reshape(-1, stacked.shape[-1]), kernel, preferred_element_type=jnp.float32)
        + conv_bias
    )
    normed = linear * lax.rsqrt(jnp.mean(linear * linear, -1, keepdims=True) + 1e-06) * norm_gain
    return jax.nn.silu(normed).astype(jnp.bfloat16).reshape(frames, height, breadth, -1)


def attend_block(carried, block_keys, block_values, query_heads):
    running, denominator, weighted = carried
    scores = jnp.einsum("hqd,khd->hqk", query_heads, block_keys, preferred_element_type=jnp.float32)
    scores = scores * query_heads.shape[-1] ** (-0.5)
    newmax = jnp.maximum(running, jnp.max(scores, -1))
    factor = jnp.exp(running - newmax)
    weights = jnp.exp(scores - newmax[..., None])
    denominator = denominator * factor + jnp.sum(weights, -1)
    product = jnp.einsum(
        "hqk,khd->hqd",
        weights.astype(jnp.bfloat16),
        block_values,
        preferred_element_type=jnp.float32,
    )
    weighted = weighted * factor[..., None] + product
    return (newmax, denominator, weighted)


def fold_pieces(query_heads, carried, pieces):
    key_piece, value_piece = pieces
    frames, height, breadth = (key_piece.shape[0], key_piece.shape[1], key_piece.shape[2])
    heads_here, head_width = (query_heads.shape[0], query_heads.shape[2])
    group_rows = 4

    def regroup(one_piece):
        shaped = one_piece.reshape(
            frames, height // group_rows, group_rows, breadth, heads_here, head_width
        )
        shaped = shaped.transpose(1, 0, 2, 3, 4, 5)
        return shaped.reshape(
            height // group_rows, frames * group_rows * breadth, heads_here, head_width
        )

    def advance(inner, blocks):
        return (attend_block(inner, blocks[0], blocks[1], query_heads), None)

    carried, _ = lax.scan(advance, carried, (regroup(key_piece), regroup(value_piece)))
    return carried


def on_device_gathered(
    queries,
    attn_keys,
    attn_values,
    residual,
    out_weight,
    out_gate,
    head_shift,
    head_scale,
    head_weight,
    head_bias,
    conv_weight,
    conv_bias,
    norm_gain,
):
    head_count = lax.axis_size("head")
    frames_dev = queries.shape[0]
    group_width = queries.shape[3] // head_count
    head_width = HEAD_DIM
    heads_here = group_width // head_width
    local_queries, local_keys, local_values = (
        lax.all_to_all(queries, "head", split_axis=3, concat_axis=0, tiled=True),
        lax.all_to_all(attn_keys, "head", split_axis=3, concat_axis=0, tiled=True),
        lax.all_to_all(attn_values, "head", split_axis=3, concat_axis=0, tiled=True),
    )
    frames_all, height, breadth = (
        local_queries.shape[0],
        local_queries.shape[1],
        local_queries.shape[2],
    )
    count = frames_all * height * breadth
    query_heads = local_queries.reshape(count, heads_here, head_width).transpose(1, 0, 2)
    initial = (
        jnp.full((heads_here, count), -1e30, jnp.float32),
        jnp.zeros((heads_here, count), jnp.float32),
        jnp.zeros((heads_here, count, head_width), jnp.float32),
    )
    carried = fold_pieces(
        query_heads,
        initial,
        (
            lax.all_gather(local_keys, "seq", axis=1, tiled=True),
            lax.all_gather(local_values, "seq", axis=1, tiled=True),
        ),
    )
    running, denominator, weighted = carried
    attended = (weighted / denominator[..., None]).astype(jnp.bfloat16)
    attended = attended.transpose(1, 0, 2).reshape(count, group_width)
    partial_value = jnp.dot(
        attended,
        lax.all_gather(out_weight, "seq", axis=1, tiled=True),
        preferred_element_type=jnp.float32,
    )
    partial_value = partial_value.reshape(frames_all, height, breadth, partial_value.shape[-1])
    owned = lax.psum_scatter(
        partial_value.astype(jnp.bfloat16), "head", scatter_dimension=0, tiled=True
    ).astype(jnp.float32)
    hidden = (residual.astype(jnp.float32) + out_gate * owned).astype(jnp.bfloat16)
    own_video = head_latent(hidden, head_shift, head_scale, head_weight, head_bias)
    earlier = from_behind(own_video, "head", 1)
    video = jnp.concatenate([earlier, own_video], 0)
    extended = padded_2(video, (("seq", 1),), 1)
    padded = jnp.pad(extended, ((0, 0), (0, 0), (1, 1), (0, 0)))
    features = convolve(padded, frames_dev, conv_weight, conv_bias, norm_gain)
    return (hidden, features)


MESH = pl.DeviceIdType.MESH


class Plan:
    def __init__(self, ns, nh, queries, residual, out_weight):
        self.ns, self.nh = ns, nh
        self.tokens = queries.shape[0] * queries.shape[1] * queries.shape[2]
        self.group = queries.shape[3] // nh // HEAD_DIM
        self.parts = ns // math.gcd(self.group, ns)
        self.units = self.group * self.parts // ns
        firsts = [self.units * s // self.parts for s in range(ns)]
        lasts = [(self.units * (s + 1) - 1) // self.parts for s in range(ns)]
        self.span = max(b - a + 1 for a, b in zip(firsts, lasts))
        self.clamp = self.group - self.span
        self.width = residual.shape[3]
        self.columns = out_weight.shape[1]
        self.slots = ns * nh
        self.bits = nh.bit_length() - 1

    def fits(self, queries):
        return (
            self.nh == 1 << self.bits
            and self.bits == 2
            and self.ns >= 2
            and self.tokens % 16 == 0
            and self.ns % self.parts == 0
            and self.columns % 128 == 0
            and queries.shape[0] >= 2
            and self.slots * self.tokens <= 1024
        )


def block_kernel(
    plan,
    q_hbm, k_hbm, v_hbm, res_hbm, w_hbm, hw_hbm,
    gate_ref, shift_ref, scale_ref, bias_ref,
    hidden_ref, near_ref,
    qkv, got, att, weight, res, head_w, term, *rest,
):
    p = plan
    landed = rest[: p.bits]
    final, patch, halo = rest[p.bits : p.bits + 3]
    (local_sem, own_sem, s1, r1, s3, r3, s5, r5, s6, r6, s7, r7) = rest[p.bits + 3 :]
    s = lax.axis_index("seq")
    h = lax.axis_index("head")
    here = s * p.nh + h

    def first_head(seq_index):
        return jnp.minimum(p.units * seq_index // p.parts, p.clamp)

    loads = [
        pltpu.make_async_copy(q_hbm, qkv.at[0], local_sem.at[0]),
        pltpu.make_async_copy(k_hbm, qkv.at[1], local_sem.at[1]),
        pltpu.make_async_copy(v_hbm, qkv.at[2], local_sem.at[2]),
    ]
    late = [
        pltpu.make_async_copy(w_hbm, weight, local_sem.at[3]),
        pltpu.make_async_copy(res_hbm, res, local_sem.at[4]),
        pltpu.make_async_copy(hw_hbm, head_w, local_sem.at[5]),
    ]
    for copy in loads:
        copy.start()

    offsets = [(ds, dh) for ds in range(p.ns) for dh in range(p.nh) if ds or dh]
    barrier = pltpu.get_barrier_semaphore()
    for ds, dh in offsets:
        pl.semaphore_signal(
            barrier,
            inc=1,
            device_id={"seq": lax.rem(s + ds, p.ns), "head": lax.rem(h + dh, p.nh)},
            device_id_type=MESH,
        )
    for copy in loads:
        copy.wait()
    pl.semaphore_wait(barrier, len(offsets))

    def piece(seq_index, head_index, j):
        start = (head_index * p.group + first_head(seq_index) + j) * HEAD_DIM
        return qkv.at[:, :, pl.ds(pl.multiple_of(start, HEAD_DIM), HEAD_DIM)]

    first_sends = []
    for index, (ds, dh) in enumerate(offsets):
        to_s, to_h = lax.rem(s + ds, p.ns), lax.rem(h + dh, p.nh)
        for j in range(p.span):
            copy = pltpu.make_async_remote_copy(
                src_ref=piece(to_s, to_h, j),
                dst_ref=got.at[here, j],
                send_sem=s1.at[index, j],
                recv_sem=r1.at[index, j],
                device_id={"seq": to_s, "head": to_h},
                device_id_type=MESH,
            )
            copy.start()
            first_sends.append(copy)
    own = [
        pltpu.make_async_copy(piece(s, h, j), got.at[here, j], own_sem.at[j])
        for j in range(p.span)
    ]
    for copy in own:
        copy.start()
    for copy in late:
        copy.start()
    for copy in own:
        copy.wait()
    for copy in first_sends:
        copy.wait()

    per_part = p.slots // p.parts
    base = first_head(s)
    gather = []
    for i in range(p.units):
        unit = p.units * s + i
        j = unit // p.parts - base
        part = lax.rem(unit, p.parts)
        q = got[pl.ds(part * per_part, per_part), j, 0].reshape(-1, HEAD_DIM)
        k = got[:, j, 1].reshape(-1, HEAD_DIM)
        v = got[:, j, 2].reshape(-1, HEAD_DIM)
        scores = lax.dot_general(
            q, k, (((1,), (1,)), ((), ())), preferred_element_type=jnp.float32
        )
        scores = scores * HEAD_DIM ** (-0.5)
        weights = jnp.exp(scores - jnp.max(scores, -1, keepdims=True))
        denominator = jnp.sum(weights, -1, keepdims=True)
        product = jnp.dot(weights.astype(jnp.bfloat16), v, preferred_element_type=jnp.float32)
        att[s, i] = (product / denominator).astype(jnp.bfloat16)
        for ds in range(1, p.ns):
            copy = pltpu.make_async_remote_copy(
                src_ref=att.at[s, i],
                dst_ref=att.at[s, i],
                send_sem=s3.at[ds - 1, i],
                recv_sem=r3.at[ds - 1, i],
                device_id={"seq": lax.rem(s + ds, p.ns)},
                device_id_type=MESH,
            )
            copy.start()
            gather.append(copy)
    late[0].wait()
    for copy in gather:
        copy.wait()

    per_seq = p.ns // p.parts
    for part in range(p.parts):
        picks = [g * p.parts + part for g in range(p.group)]
        rows = jnp.concatenate([att[u // p.units, u % p.units] for u in picks], axis=1)
        product = jnp.dot(rows, weight[...], preferred_element_type=jnp.float32)
        term[pl.ds(part * per_seq, per_seq)] = product.astype(jnp.bfloat16).reshape(
            (per_seq,) + term.shape[1:]
        )

    current = term
    for b in range(p.bits):
        bit = (h >> b) & 1
        peer = h + (1 - 2 * bit) * (1 << b)
        half = p.nh >> (b + 1)
        copy = pltpu.make_async_remote_copy(
            src_ref=current.at[:, :, 1 - bit] if b == 0 else current.at[:, 1 - bit],
            dst_ref=landed[b],
            send_sem=s5.at[b],
            recv_sem=r5.at[b],
            device_id={"head": peer},
            device_id_type=MESH,
        )
        copy.start()
        copy.wait()
        mine = current[:, :, bit] if b == 0 else current[:, bit]
        total = mine.astype(jnp.float32) + landed[b][...].astype(jnp.float32)
        landed[b][...] = total.astype(jnp.bfloat16)
        current = landed[b]

    owner = []
    for ds in range(1, p.ns):
        to_s = lax.rem(s + ds, p.ns)
        copy = pltpu.make_async_remote_copy(
            src_ref=current.at[to_s],
            dst_ref=final.at[s],
            send_sem=s6.at[ds - 1],
            recv_sem=r6.at[ds - 1],
            device_id={"seq": to_s},
            device_id_type=MESH,
        )
        copy.start()
        owner.append(copy)
    final[s] = current[s]
    for copy in late[1:]:
        copy.wait()
    for copy in owner:
        copy.wait()

    sums = jnp.zeros((p.tokens, 1), jnp.float32)
    for j in range(p.ns):
        cols = pl.ds(j * p.columns, p.columns)
        value = res[:, cols].astype(jnp.float32) + gate_ref[:, cols] * final[j].astype(jnp.float32)
        value = value.astype(jnp.bfloat16)
        hidden_ref[:, cols] = value
        sums = sums + jnp.sum(value.astype(jnp.float32), -1, keepdims=True)
    mean = sums / p.width
    center = hidden_ref[...].astype(jnp.float32) - mean
    spread = jnp.mean(center * center, -1, keepdims=True)
    normed = center * lax.rsqrt(spread + 1e-06) * (1.0 + scale_ref[...]) + shift_ref[...]
    values = jnp.dot(
        normed.astype(jnp.bfloat16), head_w[...], preferred_element_type=jnp.float32
    )
    values = (values + bias_ref[...]).astype(jnp.bfloat16)
    features = values.shape[-1]
    patch[...] = jnp.zeros_like(patch)
    patch[:, :features] = values

    moves = [(0, 1), (0, -1), (1, 0), (1, 1), (1, -1)]

    def edge(index, sign):
        dh, ds = moves[index]
        return (
            (h + sign * dh >= 0) & (h + sign * dh < p.nh)
            & (s + sign * ds >= 0) & (s + sign * ds < p.ns)
        )

    def hop(index):
        dh, ds = moves[index]
        return pltpu.make_async_remote_copy(
            src_ref=patch,
            dst_ref=halo.at[index],
            send_sem=s7.at[index],
            recv_sem=r7.at[index],
            device_id={"seq": lax.rem(s + ds + p.ns, p.ns), "head": lax.rem(h + dh, p.nh)},
            device_id_type=MESH,
        )

    for index in range(len(moves)):

        @pl.when(edge(index, 1))
        def _():
            hop(index).start()

    near_ref[1, 1] = values
    for index, (dh, ds) in enumerate(moves):

        @pl.when(edge(index, -1))
        def _():
            hop(index).wait_recv()
            near_ref[1 - dh, 1 - ds] = halo[index][:, :features]

        @pl.when(jnp.logical_not(edge(index, -1)))
        def _():
            near_ref[1 - dh, 1 - ds] = jnp.zeros_like(values)

    for index in range(len(moves)):

        @pl.when(edge(index, 1))
        def _():
            hop(index).wait_send()


def on_device(
    queries,
    attn_keys,
    attn_values,
    residual,
    out_weight,
    out_gate,
    head_shift,
    head_scale,
    head_weight,
    head_bias,
    conv_weight,
    conv_bias,
    norm_gain,
):
    ns, nh = lax.axis_size("seq"), lax.axis_size("head")
    p = Plan(ns, nh, queries, residual, out_weight)
    if not p.fits(queries):
        return on_device_gathered(
            queries, attn_keys, attn_values, residual, out_weight, out_gate, head_shift,
            head_scale, head_weight, head_bias, conv_weight, conv_bias, norm_gain,
        )
    frames, height, breadth, inner = queries.shape
    t, width, patch_size = p.tokens, p.width, head_weight.shape[1]
    dma, bf16 = pltpu.SemaphoreType.DMA, jnp.bfloat16
    tail = (t, p.columns)
    lanes = -(-patch_size // 128) * 128
    any_spec = pl.BlockSpec(memory_space=pl.ANY)
    vmem = pl.BlockSpec(memory_space=pltpu.VMEM)
    landed = [
        pltpu.VMEM((ns,) + ((nh >> 1,) if b == 0 and nh > 2 else ()) + tail, bf16)
        for b in range(p.bits)
    ]
    hidden, near = pl.pallas_call(
        functools.partial(block_kernel, p),
        out_shape=(
            jax.ShapeDtypeStruct((t, width), bf16),
            jax.ShapeDtypeStruct((2, 3, t, patch_size), bf16),
        ),
        in_specs=[any_spec] * 6 + [vmem] * 4,
        out_specs=(vmem, vmem),
        scratch_shapes=[
            pltpu.VMEM((3, t, inner), bf16),
            pltpu.VMEM((p.slots, p.span, 3, t, HEAD_DIM), bf16),
            pltpu.VMEM((ns, p.units, p.slots // p.parts * t, HEAD_DIM), bf16),
            pltpu.VMEM(out_weight.shape, bf16),
            pltpu.VMEM((t, width), bf16),
            pltpu.VMEM(head_weight.shape, bf16),
            pltpu.VMEM((ns, nh >> 1, 2) + tail, bf16),
            *landed,
            pltpu.VMEM((ns,) + tail, bf16),
            pltpu.VMEM((t, lanes), bf16),
            pltpu.VMEM((5, t, lanes), bf16),
            dma((6,)),
            dma((p.span,)),
            dma((p.slots - 1, p.span)),
            dma((p.slots - 1, p.span)),
            dma((ns - 1, p.units)),
            dma((ns - 1, p.units)),
            dma((p.bits,)),
            dma((p.bits,)),
            dma((ns - 1,)),
            dma((ns - 1,)),
            dma((5,)),
            dma((5,)),
        ],
        compiler_params=pltpu.CompilerParams(
            collective_id=0, has_side_effects=True, vmem_limit_bytes=40 * 1024 * 1024
        ),
    )(
        queries.reshape(t, inner),
        attn_keys.reshape(t, inner),
        attn_values.reshape(t, inner),
        residual.reshape(t, width),
        out_weight,
        head_weight,
        out_gate.reshape(1, -1),
        head_shift.reshape(1, -1),
        head_scale.reshape(1, -1),
        head_bias.reshape(1, -1),
    )
    channels = patch_size // 4
    video = near.reshape(2, 3, frames, height, breadth, 2, 2, channels)
    video = video.transpose(0, 2, 1, 3, 5, 4, 6, 7)
    video = video.reshape(2, frames, 3 * height * 2, breadth * 2, channels)
    video = jnp.concatenate([video[0, -2:], video[1]], 0)
    rows = height * 2
    video = video[:, rows - 1 : 2 * rows + 1]
    padded = jnp.pad(video, ((0, 0), (0, 0), (1, 1), (0, 0)))
    features = convolve(padded, frames, conv_weight, conv_bias, norm_gain)
    return (hidden.reshape(residual.shape), features)


def solution(mesh):
    return jax.shard_map(
        on_device,
        mesh=mesh,
        in_specs=(
            P(("clip", "head"), "seq", None, None),
            P(("clip", "head"), "seq", None, None),
            P(("clip", "head"), "seq", None, None),
            P(("clip", "head"), "seq", None, None),
            P("head", "seq"),
            P(),
            P(),
            P(),
            P(),
            P(),
            P(),
            P(),
            P(),
        ),
        out_specs=(P(("clip", "head"), "seq", None, None), P(("clip", "head"), "seq", None, None)),
        check_vma=False,
    )
```

```python
import functools
import math

import jax
import jax.numpy as jnp
from jax import lax
from jax.experimental import pallas as pl
from jax.experimental.pallas import tpu as pltpu
from jax.sharding import PartitionSpec as P

HEAD_DIM = 128


def from_behind(value, axis, steps):
    count = lax.axis_size(axis)
    first, last = (max(0, -steps), min(count, count - steps))
    return lax.ppermute(value, axis, [(source, source + steps) for source in range(first, last)])


def padded_2(x, sides, width):
    for axis, dim in sides:
        peers, length = (lax.axis_size(axis), x.shape[dim])
        up = [(i, (i + 1) % peers) for i in range(peers - 1)]
        down = [(j, i) for i, j in up]
        last = lax.slice_in_dim(x, length - width, length, axis=dim)
        first = lax.slice_in_dim(x, 0, width, axis=dim)
        before = lax.ppermute(last, axis, up)
        after = lax.ppermute(first, axis, down)
        x = jnp.concatenate([before, x, after], axis=dim)
    return x


def head_latent(hidden, head_shift, head_scale, head_weight, head_bias):
    values = hidden.astype(jnp.float32)
    center = values - jnp.mean(values, -1, keepdims=True)
    spread = jnp.mean(center * center, -1, keepdims=True)
    normed = (center * lax.rsqrt(spread + 1e-06) * (1.0 + head_scale) + head_shift).astype(
        jnp.bfloat16
    )
    flat = normed.reshape(-1, normed.shape[-1])
    latent = (jnp.dot(flat, head_weight, preferred_element_type=jnp.float32) + head_bias).astype(
        jnp.bfloat16
    )
    frames, height, breadth = (hidden.shape[0], hidden.shape[1], hidden.shape[2])
    channels = head_weight.shape[1] // 4
    patches = latent.reshape(frames, height, breadth, 2, 2, channels).transpose(0, 1, 3, 2, 4, 5)
    return patches.reshape(frames, height * 2, breadth * 2, channels)


def convolve(padded, frames, conv_weight, conv_bias, norm_gain):
    height = padded.shape[1] - 2
    breadth = padded.shape[2] - 2
    stacked = jnp.concatenate(
        [
            padded[
                time_off : time_off + frames,
                row_off : row_off + height,
                col_off : col_off + breadth,
            ]
            for time_off in range(3)
            for row_off in range(3)
            for col_off in range(3)
        ],
        -1,
    )
    kernel = conv_weight.reshape(-1, conv_weight.shape[-1])
    linear = (
        jnp.dot(stacked.reshape(-1, stacked.shape[-1]), kernel, preferred_element_type=jnp.float32)
        + conv_bias
    )
    normed = linear * lax.rsqrt(jnp.mean(linear * linear, -1, keepdims=True) + 1e-06) * norm_gain
    return jax.nn.silu(normed).astype(jnp.bfloat16).reshape(frames, height, breadth, -1)


def attend_block(carried, block_keys, block_values, query_heads):
    running, denominator, weighted = carried
    scores = jnp.einsum("hqd,khd->hqk", query_heads, block_keys, preferred_element_type=jnp.float32)
    scores = scores * query_heads.shape[-1] ** (-0.5)
    newmax = jnp.maximum(running, jnp.max(scores, -1))
    factor = jnp.exp(running - newmax)
    weights = jnp.exp(scores - newmax[..., None])
    denominator = denominator * factor + jnp.sum(weights, -1)
    product = jnp.einsum(
        "hqk,khd->hqd",
        weights.astype(jnp.bfloat16),
        block_values,
        preferred_element_type=jnp.float32,
    )
    weighted = weighted * factor[..., None] + product
    return (newmax, denominator, weighted)


def fold_pieces(query_heads, carried, pieces):
    key_piece, value_piece = pieces
    frames, height, breadth = (key_piece.shape[0], key_piece.shape[1], key_piece.shape[2])
    heads_here, head_width = (query_heads.shape[0], query_heads.shape[2])
    group_rows = 4

    def regroup(one_piece):
        shaped = one_piece.reshape(
            frames, height // group_rows, group_rows, breadth, heads_here, head_width
        )
        shaped = shaped.transpose(1, 0, 2, 3, 4, 5)
        return shaped.reshape(
            height // group_rows, frames * group_rows * breadth, heads_here, head_width
        )

    def advance(inner, blocks):
        return (attend_block(inner, blocks[0], blocks[1], query_heads), None)

    carried, _ = lax.scan(advance, carried, (regroup(key_piece), regroup(value_piece)))
    return carried


def on_device_gathered(
    queries,
    attn_keys,
    attn_values,
    residual,
    out_weight,
    out_gate,
    head_shift,
    head_scale,
    head_weight,
    head_bias,
    conv_weight,
    conv_bias,
    norm_gain,
):
    head_count = lax.axis_size("head")
    frames_dev = queries.shape[0]
    group_width = queries.shape[3] // head_count
    head_width = HEAD_DIM
    heads_here = group_width // head_width
    local_queries, local_keys, local_values = (
        lax.all_to_all(queries, "head", split_axis=3, concat_axis=0, tiled=True),
        lax.all_to_all(attn_keys, "head", split_axis=3, concat_axis=0, tiled=True),
        lax.all_to_all(attn_values, "head", split_axis=3, concat_axis=0, tiled=True),
    )
    frames_all, height, breadth = (
        local_queries.shape[0],
        local_queries.shape[1],
        local_queries.shape[2],
    )
    count = frames_all * height * breadth
    query_heads = local_queries.reshape(count, heads_here, head_width).transpose(1, 0, 2)
    initial = (
        jnp.full((heads_here, count), -1e30, jnp.float32),
        jnp.zeros((heads_here, count), jnp.float32),
        jnp.zeros((heads_here, count, head_width), jnp.float32),
    )
    carried = fold_pieces(
        query_heads,
        initial,
        (
            lax.all_gather(local_keys, "seq", axis=1, tiled=True),
            lax.all_gather(local_values, "seq", axis=1, tiled=True),
        ),
    )
    running, denominator, weighted = carried
    attended = (weighted / denominator[..., None]).astype(jnp.bfloat16)
    attended = attended.transpose(1, 0, 2).reshape(count, group_width)
    partial_value = jnp.dot(
        attended,
        lax.all_gather(out_weight, "seq", axis=1, tiled=True),
        preferred_element_type=jnp.float32,
    )
    partial_value = partial_value.reshape(frames_all, height, breadth, partial_value.shape[-1])
    owned = lax.psum_scatter(
        partial_value.astype(jnp.bfloat16), "head", scatter_dimension=0, tiled=True
    ).astype(jnp.float32)
    hidden = (residual.astype(jnp.float32) + out_gate * owned).astype(jnp.bfloat16)
    own_video = head_latent(hidden, head_shift, head_scale, head_weight, head_bias)
    earlier = from_behind(own_video, "head", 1)
    video = jnp.concatenate([earlier, own_video], 0)
    extended = padded_2(video, (("seq", 1),), 1)
    padded = jnp.pad(extended, ((0, 0), (0, 0), (1, 1), (0, 0)))
    features = convolve(padded, frames_dev, conv_weight, conv_bias, norm_gain)
    return (hidden, features)


MESH = pl.DeviceIdType.MESH


class Plan:
    def __init__(self, ns, nh, queries, residual, out_weight):
        self.ns, self.nh = ns, nh
        self.tokens = queries.shape[0] * queries.shape[1] * queries.shape[2]
        self.group = queries.shape[3] // nh // HEAD_DIM
        self.parts = ns // math.gcd(self.group, ns)
        self.units = self.group * self.parts // ns
        self.width = residual.shape[3]
        self.columns = out_weight.shape[1]
        self.slots = ns * nh
        self.chunk = 256 if self.columns % 256 == 0 else 128
        self.chunks = self.columns // self.chunk
        self.bits = nh.bit_length() - 1

    def fits(self, queries):
        return (
            self.nh == 1 << self.bits
            and self.bits == 2
            and self.ns % 2 == 0
            and self.parts == 2
            and self.units == 3
            and self.tokens % 16 == 0
            and self.columns % 128 == 0
            and queries.shape[0] >= 2
            and self.slots * self.tokens <= 1024
        )


def block_kernel(
    plan,
    q_hbm, k_hbm, v_hbm, res_hbm, w_hbm, hw_hbm,
    gate_ref, shift_ref, scale_ref, bias_ref,
    hidden_ref, near_ref,
    qkv, got, att, weight, res, head_w, term, *rest,
):
    p = plan
    landed = rest[: p.bits]
    final, patch, halo = rest[p.bits : p.bits + 3]
    (local_sem, own_sem, s1, r1, sf, rf, s3, r3, s5, r5, s6, r6, s7, r7) = rest[p.bits + 3 :]
    s = lax.axis_index("seq")
    h = lax.axis_index("head")
    here = s * p.nh + h

    loads = [
        pltpu.make_async_copy(q_hbm, qkv.at[0], local_sem.at[0]),
        pltpu.make_async_copy(k_hbm, qkv.at[1], local_sem.at[1]),
        pltpu.make_async_copy(v_hbm, qkv.at[2], local_sem.at[2]),
    ]
    late = [
        pltpu.make_async_copy(w_hbm, weight, local_sem.at[3]),
        pltpu.make_async_copy(res_hbm, res, local_sem.at[4]),
        pltpu.make_async_copy(hw_hbm, head_w, local_sem.at[5]),
    ]
    for copy in loads:
        copy.start()

    offsets = [(ds, dh) for ds in range(p.ns) for dh in range(p.nh) if ds or dh]
    barrier = pltpu.get_barrier_semaphore()
    for ds, dh in offsets:
        pl.semaphore_signal(
            barrier,
            inc=1,
            device_id={"seq": lax.rem(s + ds, p.ns), "head": lax.rem(h + dh, p.nh)},
            device_id_type=MESH,
        )
    for copy in loads:
        copy.wait()
    pl.semaphore_wait(barrier, len(offsets))

    def piece(seq_index, head_index, j):
        start = (head_index * p.group + 3 * (seq_index // 2) + seq_index % 2 + j) * HEAD_DIM
        return qkv.at[:, :, pl.ds(pl.multiple_of(start, HEAD_DIM), HEAD_DIM)]

    def place(seq_index, k):
        return 1 - seq_index % 2 if k == 0 else seq_index % 2

    def direct(source, target):
        up = (source // 2 < target // 2) & (target % 2 == 1)
        down = (source // 2 > target // 2) & (target % 2 == 0)
        return jnp.logical_not(up | down)

    def first_hop(index, k, to_s, to_h, slot, j):
        return pltpu.make_async_remote_copy(
            src_ref=piece(to_s, to_h, j),
            dst_ref=got.at[slot, j],
            send_sem=s1.at[index, k],
            recv_sem=r1.at[index, k],
            device_id={"seq": to_s, "head": to_h},
            device_id_type=MESH,
        )

    def sending(index, k):
        ds, dh = offsets[index]
        to_s, to_h = lax.rem(s + ds, p.ns), lax.rem(h + dh, p.nh)
        return to_s, first_hop(index, k, to_s, to_h, here, place(to_s, k))

    def arriving(index, k):
        ds, dh = offsets[index]
        from_s, from_h = lax.rem(s - ds + p.ns, p.ns), lax.rem(h - dh + p.nh, p.nh)
        return from_s, first_hop(index, k, s, h, from_s * p.nh + from_h, place(s, k))

    def guarded(k, ds, source, target, act):
        if k == 0 and ds:
            pl.when(direct(source, target))(act)
        else:
            act()

    for k in range(2):
        for index, (ds, dh) in enumerate(offsets):
            to_s, copy = sending(index, k)
            guarded(k, ds, s, to_s, copy.start)
    own = [
        pltpu.make_async_copy(piece(s, h, j), got.at[here, j], own_sem.at[j]) for j in range(2)
    ]
    for copy in own:
        copy.start()
    for copy in late:
        copy.start()
    for copy in own:
        copy.wait()

    even = s % 2 == 0
    peer_s = s + 1 - 2 * (s % 2)

    def hand_on(level, j_from, j_to):
        rows = pl.ds(level * p.nh, p.nh)
        return pltpu.make_async_remote_copy(
            src_ref=got.at[rows, j_from, pl.ds(1, 2)],
            dst_ref=got.at[rows, j_to, pl.ds(1, 2)],
            send_sem=sf.at[level],
            recv_sem=rf.at[level],
            device_id={"seq": peer_s},
            device_id_type=MESH,
        )

    def handed(level):
        return jnp.where(even, level // 2 < s // 2, level // 2 > s // 2)

    def expected(level):
        return jnp.where(even, level // 2 > s // 2, level // 2 < s // 2)

    for ds in list(range(1, p.ns)) + [0]:
        for index, (ds2, dh) in enumerate(offsets):
            if ds2 == ds:
                from_s, copy = arriving(index, 0)
                guarded(0, ds, from_s, s, copy.wait_recv)
        if ds:
            level = lax.rem(s - ds + p.ns, p.ns)

            @pl.when(handed(level))
            def _():
                hand_on(level, place(s, 0), place(peer_s, 0)).start()

    for index in range(len(offsets)):
        arriving(index, 1)[1].wait_recv()

    per_part = p.slots // p.parts

    def gather_hop(source, i, step):
        return pltpu.make_async_remote_copy(
            src_ref=att.at[source, i],
            dst_ref=att.at[source, i],
            send_sem=s3.at[(step + 1) // 2, source, i],
            recv_sem=r3.at[source, i],
            device_id={"seq": lax.rem(s + step + p.ns, p.ns)},
            device_id_type=MESH,
        )

    up_open, down_open = s + 1 < p.ns, s > 0
    for i in range(p.units):
        j = place(s, 1) if i < 2 else place(s, 0)
        part = i if i < 2 else s % 2
        if i == 2:
            for ds in range(1, p.ns):
                level = lax.rem(s - ds + p.ns, p.ns)

                @pl.when(expected(level))
                def _():
                    hand_on(level, place(peer_s, 0), place(s, 0)).wait_recv()

        q = got[pl.ds(part * per_part, per_part), j, 0].reshape(-1, HEAD_DIM)
        k = got[:, j, 1].reshape(-1, HEAD_DIM)
        v = got[:, j, 2].reshape(-1, HEAD_DIM)
        scores = lax.dot_general(
            q, k, (((1,), (1,)), ((), ())), preferred_element_type=jnp.float32
        )
        scores = scores * HEAD_DIM ** (-0.5)
        weights = jnp.exp(scores - jnp.max(scores, -1, keepdims=True))
        denominator = jnp.sum(weights, -1, keepdims=True)
        product = jnp.dot(weights.astype(jnp.bfloat16), v, preferred_element_type=jnp.float32)
        att[s, i] = (product / denominator).astype(jnp.bfloat16)
        pl.when(up_open)(gather_hop(s, i, 1).start)
        pl.when(down_open)(gather_hop(s, i, -1).start)

    late[0].wait()
    for distance in range(1, p.ns):
        for i in range(p.units):

            @pl.when(s - distance >= 0)
            def _():
                gather_hop(s - distance, i, 1).wait_recv()
                pl.when(up_open)(gather_hop(s - distance, i, 1).start)

            @pl.when(s + distance < p.ns)
            def _():
                gather_hop(s + distance, i, -1).wait_recv()
                pl.when(down_open)(gather_hop(s + distance, i, -1).start)

    def halving(c, b):
        bit = (h >> b) & 1
        source = term.at[c, :, :, 1 - bit] if b == 0 else landed[b - 1].at[c, :, 1 - bit]
        return pltpu.make_async_remote_copy(
            src_ref=source,
            dst_ref=landed[b].at[c],
            send_sem=s5.at[b, c],
            recv_sem=r5.at[b, c],
            device_id={"head": h + (1 - 2 * bit) * (1 << b)},
            device_id_type=MESH,
        )

    per_seq = p.ns // p.parts
    rows = []
    for part in range(p.parts):
        picks = [
            att[2 * (g // 3) + part, 2] if g % 3 == 1 else att[2 * (g // 3) + g % 3 // 2, part]
            for g in range(p.group)
        ]
        rows.append(jnp.concatenate(picks, axis=1))
    for c in range(p.chunks):
        cols = pl.ds(c * p.chunk, p.chunk)
        for part in range(p.parts):
            product = jnp.dot(rows[part], weight[:, cols], preferred_element_type=jnp.float32)
            term[c, pl.ds(part * per_seq, per_seq)] = product.astype(jnp.bfloat16).reshape(
                (per_seq,) + term.shape[2:]
            )
        halving(c, 0).start()

    def add_up(c, b):
        bit = (h >> b) & 1
        mine = term[c, :, :, bit] if b == 0 else landed[b - 1][c, :, bit]
        total = mine.astype(jnp.float32) + landed[b][c].astype(jnp.float32)
        landed[b][c] = total.astype(jnp.bfloat16)

    for b in range(p.bits - 1):
        for c in range(p.chunks):
            halving(c, b).wait_recv()
            add_up(c, b)
            halving(c, b + 1).start()
    summed = landed[p.bits - 1]

    def to_owner(c, ds, slot):
        to_s = lax.rem(s + ds, p.ns)
        return pltpu.make_async_remote_copy(
            src_ref=summed.at[c, to_s],
            dst_ref=final.at[c, slot],
            send_sem=s6.at[ds - 1, c],
            recv_sem=r6.at[ds - 1, c],
            device_id={"seq": to_s},
            device_id_type=MESH,
        )

    for c in range(p.chunks):
        halving(c, p.bits - 1).wait_recv()
        add_up(c, p.bits - 1)
        for ds in range(1, p.ns):
            to_owner(c, ds, s).start()
        final[c, s] = summed[c, s]
    for copy in late[1:]:
        copy.wait()

    sums = jnp.zeros((p.tokens, 1), jnp.float32)
    for c in range(p.chunks):
        for ds in range(1, p.ns):
            to_owner(c, ds, lax.rem(s - ds + p.ns, p.ns)).wait_recv()
        for j in range(p.ns):
            cols = pl.ds(j * p.columns + c * p.chunk, p.chunk)
            added = gate_ref[:, cols] * final[c, j].astype(jnp.float32)
            value = (res[:, cols].astype(jnp.float32) + added).astype(jnp.bfloat16)
            hidden_ref[:, cols] = value
            sums = sums + jnp.sum(value.astype(jnp.float32), -1, keepdims=True)
    mean = sums / p.width
    center = hidden_ref[...].astype(jnp.float32) - mean
    spread = jnp.mean(center * center, -1, keepdims=True)
    normed = center * lax.rsqrt(spread + 1e-06) * (1.0 + scale_ref[...]) + shift_ref[...]
    values = lax.dot_general(
        normed.astype(jnp.bfloat16),
        head_w[...],
        (((1,), (1,)), ((), ())),
        preferred_element_type=jnp.float32,
    )
    values = (values + bias_ref[...]).astype(jnp.bfloat16)
    features = values.shape[-1]
    patch[...] = jnp.zeros_like(patch)
    patch[:, :features] = values

    moves = [(0, 1), (0, -1), (1, 0), (1, 1), (1, -1)]

    def edge(index, sign):
        dh, ds = moves[index]
        return (
            (h + sign * dh >= 0) & (h + sign * dh < p.nh)
            & (s + sign * ds >= 0) & (s + sign * ds < p.ns)
        )

    def hop(index):
        dh, ds = moves[index]
        return pltpu.make_async_remote_copy(
            src_ref=patch,
            dst_ref=halo.at[index],
            send_sem=s7.at[index],
            recv_sem=r7.at[index],
            device_id={"seq": lax.rem(s + ds + p.ns, p.ns), "head": lax.rem(h + dh, p.nh)},
            device_id_type=MESH,
        )

    for index in range(len(moves)):

        @pl.when(edge(index, 1))
        def _():
            hop(index).start()

    near_ref[1, 1] = values
    for index, (dh, ds) in enumerate(moves):

        @pl.when(edge(index, -1))
        def _():
            hop(index).wait_recv()
            near_ref[1 - dh, 1 - ds] = halo[index][:, :features]

        @pl.when(jnp.logical_not(edge(index, -1)))
        def _():
            near_ref[1 - dh, 1 - ds] = jnp.zeros_like(values)

    for index in range(len(moves)):

        @pl.when(edge(index, 1))
        def _():
            hop(index).wait_send()

    for k in range(2):
        for index, (ds, dh) in enumerate(offsets):
            to_s, copy = sending(index, k)
            guarded(k, ds, s, to_s, copy.wait_send)
    for ds in range(1, p.ns):
        level = lax.rem(s - ds + p.ns, p.ns)

        @pl.when(handed(level))
        def _():
            hand_on(level, place(s, 0), place(peer_s, 0)).wait_send()

    for distance in range(p.ns):
        for i in range(p.units):

            @pl.when((s - distance >= 0) & up_open)
            def _():
                gather_hop(s - distance, i, 1).wait_send()

            @pl.when((s + distance < p.ns) & down_open)
            def _():
                gather_hop(s + distance, i, -1).wait_send()

    for c in range(p.chunks):
        for b in range(p.bits):
            halving(c, b).wait_send()
        for ds in range(1, p.ns):
            to_owner(c, ds, s).wait_send()


def on_device(
    queries,
    attn_keys,
    attn_values,
    residual,
    out_weight,
    out_gate,
    head_shift,
    head_scale,
    head_weight,
    head_bias,
    conv_weight,
    conv_bias,
    norm_gain,
):
    ns, nh = lax.axis_size("seq"), lax.axis_size("head")
    p = Plan(ns, nh, queries, residual, out_weight)
    if not p.fits(queries):
        return on_device_gathered(
            queries, attn_keys, attn_values, residual, out_weight, out_gate, head_shift,
            head_scale, head_weight, head_bias, conv_weight, conv_bias, norm_gain,
        )
    frames, height, breadth, inner = queries.shape
    t, width, patch_size = p.tokens, p.width, head_weight.shape[1]
    dma, bf16 = pltpu.SemaphoreType.DMA, jnp.bfloat16
    tail = (t, p.chunk)
    lanes = -(-patch_size // 128) * 128
    any_spec = pl.BlockSpec(memory_space=pl.ANY)
    vmem = pl.BlockSpec(memory_space=pltpu.VMEM)
    landed = [
        pltpu.VMEM((p.chunks, ns) + ((nh >> 1,) if b == 0 and nh > 2 else ()) + tail, bf16)
        for b in range(p.bits)
    ]
    hidden, near = pl.pallas_call(
        functools.partial(block_kernel, p),
        out_shape=(
            jax.ShapeDtypeStruct((t, width), bf16),
            jax.ShapeDtypeStruct((2, 3, t, patch_size), bf16),
        ),
        in_specs=[any_spec] * 6 + [vmem] * 4,
        out_specs=(vmem, vmem),
        scratch_shapes=[
            pltpu.VMEM((3, t, inner), bf16),
            pltpu.VMEM((p.slots, 2, 3, t, HEAD_DIM), bf16),
            pltpu.VMEM((ns, p.units, p.slots // p.parts * t, HEAD_DIM), bf16),
            pltpu.VMEM(out_weight.shape, bf16),
            pltpu.VMEM((t, width), bf16),
            pltpu.VMEM(head_weight.shape[::-1], bf16),
            pltpu.VMEM((p.chunks, ns, nh >> 1, 2) + tail, bf16),
            *landed,
            pltpu.VMEM((p.chunks, ns) + tail, bf16),
            pltpu.VMEM((t, lanes), bf16),
            pltpu.VMEM((5, t, lanes), bf16),
            dma((6,)),
            dma((2,)),
            dma((p.slots - 1, 2)),
            dma((p.slots - 1, 2)),
            dma((ns,)),
            dma((ns,)),
            dma((2, ns, p.units)),
            dma((ns, p.units)),
            dma((p.bits, p.chunks)),
            dma((p.bits, p.chunks)),
            dma((ns - 1, p.chunks)),
            dma((ns - 1, p.chunks)),
            dma((5,)),
            dma((5,)),
        ],
        compiler_params=pltpu.CompilerParams(
            collective_id=0, has_side_effects=True, vmem_limit_bytes=60 * 1024 * 1024
        ),
    )(
        queries.reshape(t, inner),
        attn_keys.reshape(t, inner),
        attn_values.reshape(t, inner),
        residual.reshape(t, width),
        out_weight,
        head_weight.T,
        out_gate.reshape(1, -1),
        head_shift.reshape(1, -1),
        head_scale.reshape(1, -1),
        head_bias.reshape(1, -1),
    )
    channels = patch_size // 4
    video = near.reshape(2, 3, frames, height, breadth, 2, 2, channels)
    video = video.transpose(0, 2, 1, 3, 5, 4, 6, 7)
    video = video.reshape(2, frames, 3 * height * 2, breadth * 2, channels)
    video = jnp.concatenate([video[0, -2:], video[1]], 0)
    rows = height * 2
    video = video[:, rows - 1 : 2 * rows + 1]
    padded = jnp.pad(video, ((0, 0), (0, 0), (1, 1), (0, 0)))
    features = convolve(padded, frames, conv_weight, conv_bias, norm_gain)
    return (hidden.reshape(residual.shape), features)


def solution(mesh):
    return jax.shard_map(
        on_device,
        mesh=mesh,
        in_specs=(
            P(("clip", "head"), "seq", None, None),
            P(("clip", "head"), "seq", None, None),
            P(("clip", "head"), "seq", None, None),
            P(("clip", "head"), "seq", None, None),
            P("head", "seq"),
            P(),
            P(),
            P(),
            P(),
            P(),
            P(),
            P(),
            P(),
        ),
        out_specs=(P(("clip", "head"), "seq", None, None), P(("clip", "head"), "seq", None, None)),
        check_vma=False,
    )
```

```python
import functools
import math

import jax
import jax.numpy as jnp
from jax import lax
from jax.experimental import pallas as pl
from jax.experimental.pallas import tpu as pltpu
from jax.sharding import PartitionSpec as P

HEAD_DIM = 128


def from_behind(value, axis, steps):
    count = lax.axis_size(axis)
    first, last = (max(0, -steps), min(count, count - steps))
    return lax.ppermute(value, axis, [(source, source + steps) for source in range(first, last)])


def padded_2(x, sides, width):
    for axis, dim in sides:
        peers, length = (lax.axis_size(axis), x.shape[dim])
        up = [(i, (i + 1) % peers) for i in range(peers - 1)]
        down = [(j, i) for i, j in up]
        last = lax.slice_in_dim(x, length - width, length, axis=dim)
        first = lax.slice_in_dim(x, 0, width, axis=dim)
        before = lax.ppermute(last, axis, up)
        after = lax.ppermute(first, axis, down)
        x = jnp.concatenate([before, x, after], axis=dim)
    return x


def head_latent(hidden, head_shift, head_scale, head_weight, head_bias):
    values = hidden.astype(jnp.float32)
    center = values - jnp.mean(values, -1, keepdims=True)
    spread = jnp.mean(center * center, -1, keepdims=True)
    normed = (center * lax.rsqrt(spread + 1e-06) * (1.0 + head_scale) + head_shift).astype(
        jnp.bfloat16
    )
    flat = normed.reshape(-1, normed.shape[-1])
    latent = (jnp.dot(flat, head_weight, preferred_element_type=jnp.float32) + head_bias).astype(
        jnp.bfloat16
    )
    frames, height, breadth = (hidden.shape[0], hidden.shape[1], hidden.shape[2])
    channels = head_weight.shape[1] // 4
    patches = latent.reshape(frames, height, breadth, 2, 2, channels).transpose(0, 1, 3, 2, 4, 5)
    return patches.reshape(frames, height * 2, breadth * 2, channels)


def convolve(padded, frames, conv_weight, conv_bias, norm_gain):
    height = padded.shape[1] - 2
    breadth = padded.shape[2] - 2
    stacked = jnp.concatenate(
        [
            padded[
                time_off : time_off + frames,
                row_off : row_off + height,
                col_off : col_off + breadth,
            ]
            for time_off in range(3)
            for row_off in range(3)
            for col_off in range(3)
        ],
        -1,
    )
    kernel = conv_weight.reshape(-1, conv_weight.shape[-1])
    linear = (
        jnp.dot(stacked.reshape(-1, stacked.shape[-1]), kernel, preferred_element_type=jnp.float32)
        + conv_bias
    )
    normed = linear * lax.rsqrt(jnp.mean(linear * linear, -1, keepdims=True) + 1e-06) * norm_gain
    return jax.nn.silu(normed).astype(jnp.bfloat16).reshape(frames, height, breadth, -1)


def attend_block(carried, block_keys, block_values, query_heads):
    running, denominator, weighted = carried
    scores = jnp.einsum("hqd,khd->hqk", query_heads, block_keys, preferred_element_type=jnp.float32)
    scores = scores * query_heads.shape[-1] ** (-0.5)
    newmax = jnp.maximum(running, jnp.max(scores, -1))
    factor = jnp.exp(running - newmax)
    weights = jnp.exp(scores - newmax[..., None])
    denominator = denominator * factor + jnp.sum(weights, -1)
    product = jnp.einsum(
        "hqk,khd->hqd",
        weights.astype(jnp.bfloat16),
        block_values,
        preferred_element_type=jnp.float32,
    )
    weighted = weighted * factor[..., None] + product
    return (newmax, denominator, weighted)


def fold_pieces(query_heads, carried, pieces):
    key_piece, value_piece = pieces
    frames, height, breadth = (key_piece.shape[0], key_piece.shape[1], key_piece.shape[2])
    heads_here, head_width = (query_heads.shape[0], query_heads.shape[2])
    group_rows = 4

    def regroup(one_piece):
        shaped = one_piece.reshape(
            frames, height // group_rows, group_rows, breadth, heads_here, head_width
        )
        shaped = shaped.transpose(1, 0, 2, 3, 4, 5)
        return shaped.reshape(
            height // group_rows, frames * group_rows * breadth, heads_here, head_width
        )

    def advance(inner, blocks):
        return (attend_block(inner, blocks[0], blocks[1], query_heads), None)

    carried, _ = lax.scan(advance, carried, (regroup(key_piece), regroup(value_piece)))
    return carried


def on_device_gathered(
    queries,
    attn_keys,
    attn_values,
    residual,
    out_weight,
    out_gate,
    head_shift,
    head_scale,
    head_weight,
    head_bias,
    conv_weight,
    conv_bias,
    norm_gain,
):
    head_count = lax.axis_size("head")
    frames_dev = queries.shape[0]
    group_width = queries.shape[3] // head_count
    head_width = HEAD_DIM
    heads_here = group_width // head_width
    local_queries, local_keys, local_values = (
        lax.all_to_all(queries, "head", split_axis=3, concat_axis=0, tiled=True),
        lax.all_to_all(attn_keys, "head", split_axis=3, concat_axis=0, tiled=True),
        lax.all_to_all(attn_values, "head", split_axis=3, concat_axis=0, tiled=True),
    )
    frames_all, height, breadth = (
        local_queries.shape[0],
        local_queries.shape[1],
        local_queries.shape[2],
    )
    count = frames_all * height * breadth
    query_heads = local_queries.reshape(count, heads_here, head_width).transpose(1, 0, 2)
    initial = (
        jnp.full((heads_here, count), -1e30, jnp.float32),
        jnp.zeros((heads_here, count), jnp.float32),
        jnp.zeros((heads_here, count, head_width), jnp.float32),
    )
    carried = fold_pieces(
        query_heads,
        initial,
        (
            lax.all_gather(local_keys, "seq", axis=1, tiled=True),
            lax.all_gather(local_values, "seq", axis=1, tiled=True),
        ),
    )
    running, denominator, weighted = carried
    attended = (weighted / denominator[..., None]).astype(jnp.bfloat16)
    attended = attended.transpose(1, 0, 2).reshape(count, group_width)
    partial_value = jnp.dot(
        attended,
        lax.all_gather(out_weight, "seq", axis=1, tiled=True),
        preferred_element_type=jnp.float32,
    )
    partial_value = partial_value.reshape(frames_all, height, breadth, partial_value.shape[-1])
    owned = lax.psum_scatter(
        partial_value.astype(jnp.bfloat16), "head", scatter_dimension=0, tiled=True
    ).astype(jnp.float32)
    hidden = (residual.astype(jnp.float32) + out_gate * owned).astype(jnp.bfloat16)
    own_video = head_latent(hidden, head_shift, head_scale, head_weight, head_bias)
    earlier = from_behind(own_video, "head", 1)
    video = jnp.concatenate([earlier, own_video], 0)
    extended = padded_2(video, (("seq", 1),), 1)
    padded = jnp.pad(extended, ((0, 0), (0, 0), (1, 1), (0, 0)))
    features = convolve(padded, frames_dev, conv_weight, conv_bias, norm_gain)
    return (hidden, features)


MESH = pl.DeviceIdType.MESH


class Plan:
    def __init__(self, ns, nh, queries, residual, out_weight):
        self.ns, self.nh = ns, nh
        self.tokens = queries.shape[0] * queries.shape[1] * queries.shape[2]
        self.group = queries.shape[3] // nh // HEAD_DIM
        self.parts = ns // math.gcd(self.group, ns)
        self.units = self.group * self.parts // ns
        self.width = residual.shape[3]
        self.columns = out_weight.shape[1]
        self.slots = ns * nh
        self.chunk = 256 if self.columns % 256 == 0 else 128
        self.chunks = self.columns // self.chunk
        self.bits = nh.bit_length() - 1

    def fits(self, queries):
        return (
            self.nh == 1 << self.bits
            and self.bits == 2
            and self.ns % 2 == 0
            and self.parts == 2
            and self.units == 3
            and self.tokens % 16 == 0
            and self.columns % 128 == 0
            and queries.shape[0] >= 2
            and self.slots * self.tokens <= 1024
        )


def block_kernel(
    plan,
    q_hbm, k_hbm, v_hbm, res_hbm, w_hbm, hw_hbm,
    gate_ref, shift_ref, scale_ref, bias_ref,
    hidden_ref, near_ref,
    qkv, got, att, weight, res, head_w, term, *rest,
):
    p = plan
    landed = rest[: p.bits]
    final, patch, halo = rest[p.bits : p.bits + 3]
    (local_sem, own_sem, s1, r1, sf, rf, s3, r3, s5, r5, s6, r6, s7, r7) = rest[p.bits + 3 :]
    s = lax.axis_index("seq")
    h = lax.axis_index("head")

    loads = [
        pltpu.make_async_copy(q_hbm, qkv.at[0], local_sem.at[0]),
        pltpu.make_async_copy(k_hbm, qkv.at[1], local_sem.at[1]),
        pltpu.make_async_copy(v_hbm, qkv.at[2], local_sem.at[2]),
    ]
    late = [
        pltpu.make_async_copy(w_hbm, weight, local_sem.at[3]),
        pltpu.make_async_copy(res_hbm, res, local_sem.at[4]),
        pltpu.make_async_copy(hw_hbm, head_w, local_sem.at[5]),
    ]
    for copy in loads:
        copy.start()

    offsets = [(ds, dh) for ds in range(p.ns) for dh in range(p.nh) if ds or dh]
    barrier = pltpu.get_barrier_semaphore()
    for ds, dh in offsets:
        pl.semaphore_signal(
            barrier,
            inc=1,
            device_id={"seq": lax.rem(s + ds, p.ns), "head": lax.rem(h + dh, p.nh)},
            device_id_type=MESH,
        )
    for copy in loads:
        copy.wait()
    pl.semaphore_wait(barrier, len(offsets))

    def piece(seq_index, head_index, j):
        start = (head_index * p.group + 3 * (seq_index // 2) + seq_index % 2 + j) * HEAD_DIM
        return qkv.at[:, :, pl.ds(pl.multiple_of(start, HEAD_DIM), HEAD_DIM)]

    def place(seq_index, k):
        return 1 - seq_index % 2 if k == 0 else seq_index % 2

    def direct(source, target):
        up = (source // 2 < target // 2) & (target % 2 == 1)
        down = (source // 2 > target // 2) & (target % 2 == 0)
        return jnp.logical_not(up | down)

    def first_hop(index, k, to_s, to_h, from_s, from_h, j):
        return pltpu.make_async_remote_copy(
            src_ref=piece(to_s, to_h, j),
            dst_ref=got.at[from_h % 2, from_s, from_h // 2, j],
            send_sem=s1.at[index, k],
            recv_sem=r1.at[index, k],
            device_id={"seq": to_s, "head": to_h},
            device_id_type=MESH,
        )

    def sending(index, k):
        ds, dh = offsets[index]
        to_s, to_h = lax.rem(s + ds, p.ns), lax.rem(h + dh, p.nh)
        return to_s, first_hop(index, k, to_s, to_h, s, h, place(to_s, k))

    def arriving(index, k):
        ds, dh = offsets[index]
        from_s, from_h = lax.rem(s - ds + p.ns, p.ns), lax.rem(h - dh + p.nh, p.nh)
        return from_s, first_hop(index, k, s, h, from_s, from_h, place(s, k))

    def guarded(k, ds, source, target, act):
        if k == 0 and ds:
            pl.when(direct(source, target))(act)
        else:
            act()

    for k in range(2):
        for index, (ds, dh) in enumerate(offsets):
            to_s, copy = sending(index, k)
            guarded(k, ds, s, to_s, copy.start)
    own = [
        pltpu.make_async_copy(piece(s, h, j), got.at[h % 2, s, h // 2, j], own_sem.at[j])
        for j in range(2)
    ]
    for copy in own:
        copy.start()
    for copy in late:
        copy.start()
    for copy in own:
        copy.wait()

    even = s % 2 == 0
    peer_s = s + 1 - 2 * (s % 2)

    def hand_on(level, j_from, j_to):
        return pltpu.make_async_remote_copy(
            src_ref=got.at[:, level, :, j_from],
            dst_ref=got.at[:, level, :, j_to],
            send_sem=sf.at[level],
            recv_sem=rf.at[level],
            device_id={"seq": peer_s},
            device_id_type=MESH,
        )

    def handed(level):
        return jnp.where(even, level // 2 < s // 2, level // 2 > s // 2)

    def expected(level):
        return jnp.where(even, level // 2 > s // 2, level // 2 < s // 2)

    for ds in list(range(1, p.ns)) + [0]:
        for index, (ds2, dh) in enumerate(offsets):
            if ds2 == ds:
                from_s, copy = arriving(index, 0)
                guarded(0, ds, from_s, s, copy.wait_recv)
        if ds:
            level = lax.rem(s - ds + p.ns, p.ns)

            @pl.when(handed(level))
            def _():
                hand_on(level, place(s, 0), place(peer_s, 0)).start()


    def gather_hop(source, i, step):
        return pltpu.make_async_remote_copy(
            src_ref=att.at[source, i],
            dst_ref=att.at[source, i],
            send_sem=s3.at[(step + 1) // 2, source, i],
            recv_sem=r3.at[source, i],
            device_id={"seq": lax.rem(s + step + p.ns, p.ns)},
            device_id_type=MESH,
        )

    up_open, down_open = s + 1 < p.ns, s > 0
    order = (2, 0, 1)
    for i in order:
        j = place(s, 1) if i < 2 else place(s, 0)
        part = i if i < 2 else s % 2
        if i == 2:
            for ds in range(1, p.ns):
                level = lax.rem(s - ds + p.ns, p.ns)

                @pl.when(expected(level))
                def _():
                    hand_on(level, place(peer_s, 0), place(s, 0)).wait_recv()

        if i == 0:
            for index in range(len(offsets)):
                arriving(index, 1)[1].wait_recv()
        q = got[part, :, :, j, 0].reshape(-1, HEAD_DIM)
        k = got[:, :, :, j, 1].reshape(-1, HEAD_DIM)
        v = got[:, :, :, j, 2].reshape(-1, HEAD_DIM)
        scores = lax.dot_general(
            q, k, (((1,), (1,)), ((), ())), preferred_element_type=jnp.float32
        )
        scores = scores * HEAD_DIM ** (-0.5)
        weights = jnp.exp(scores - jnp.max(scores, -1, keepdims=True))
        denominator = jnp.sum(weights, -1, keepdims=True)
        product = jnp.dot(weights.astype(jnp.bfloat16), v, preferred_element_type=jnp.float32)
        att[s, i] = (product / denominator).astype(jnp.bfloat16)
        pl.when(up_open)(gather_hop(s, i, 1).start)
        pl.when(down_open)(gather_hop(s, i, -1).start)

    late[0].wait()

    def relay(i, distance):
        @pl.when(s - distance >= 0)
        def _():
            gather_hop(s - distance, i, 1).wait_recv()
            pl.when(up_open)(gather_hop(s - distance, i, 1).start)

        @pl.when(s + distance < p.ns)
        def _():
            gather_hop(s + distance, i, -1).wait_recv()
            pl.when(down_open)(gather_hop(s + distance, i, -1).start)

    waves = sorted(
        (position + distance, position, i, distance)
        for position, i in enumerate(order)
        for distance in range(1, p.ns)
    )
    for _, _, i, distance in waves[:-1]:
        relay(i, distance)

    def halving(c, b):
        bit = (h >> b) & 1
        source = term.at[c, 1 - bit] if b == 0 else landed[b - 1].at[c, :, 1 - bit]
        return pltpu.make_async_remote_copy(
            src_ref=source,
            dst_ref=landed[b].at[c],
            send_sem=s5.at[b, c],
            recv_sem=r5.at[b, c],
            device_id={"head": h + (1 - 2 * bit) * (1 << b)},
            device_id_type=MESH,
        )

    def add_up(c, b):
        bit = (h >> b) & 1
        mine = term[c, bit] if b == 0 else landed[b - 1][c, :, bit]
        total = mine.astype(jnp.float32) + landed[b][c].astype(jnp.float32)
        landed[b][c] = total.astype(jnp.bfloat16)

    for part in range(p.parts):
        if part == p.parts - 1:
            relay(*waves[-1][2:])
        picks = [
            att[2 * (g // 3) + part, 2] if g % 3 == 1 else att[2 * (g // 3) + g % 3 // 2, part]
            for g in range(p.group)
        ]
        rows = jnp.concatenate(picks, axis=1)
        for c in range(p.chunks):
            cols = pl.ds(c * p.chunk, p.chunk)
            product = jnp.dot(rows, weight[:, cols], preferred_element_type=jnp.float32)
            term[c, part] = product.astype(jnp.bfloat16).reshape(term.shape[2:])
            pl.when(h % 2 != part)(halving(c, 0).start)

        @pl.when(h % 2 == part)
        def _():
            for c in range(p.chunks):
                halving(c, 0).wait_recv()
                add_up(c, 0)
                halving(c, 1).start()

    summed = landed[p.bits - 1]

    def to_owner(c, ds, slot):
        to_s = lax.rem(s + ds, p.ns)
        return pltpu.make_async_remote_copy(
            src_ref=summed.at[c, to_s],
            dst_ref=final.at[c, slot],
            send_sem=s6.at[ds - 1, c],
            recv_sem=r6.at[ds - 1, c],
            device_id={"seq": to_s},
            device_id_type=MESH,
        )

    for c in range(p.chunks):
        halving(c, p.bits - 1).wait_recv()
        add_up(c, p.bits - 1)
        for ds in range(1, p.ns):
            to_owner(c, ds, s).start()
        final[c, s] = summed[c, s]
    for copy in late[1:]:
        copy.wait()

    sums = jnp.zeros((p.tokens, 1), jnp.float32)
    for c in range(p.chunks):
        for ds in range(1, p.ns):
            to_owner(c, ds, lax.rem(s - ds + p.ns, p.ns)).wait_recv()
        for j in range(p.ns):
            cols = pl.ds(j * p.columns + c * p.chunk, p.chunk)
            added = gate_ref[:, cols] * final[c, j].astype(jnp.float32)
            value = (res[:, cols].astype(jnp.float32) + added).astype(jnp.bfloat16)
            hidden_ref[:, cols] = value
            sums = sums + jnp.sum(value.astype(jnp.float32), -1, keepdims=True)
    mean = sums / p.width
    center = hidden_ref[...].astype(jnp.float32) - mean
    spread = jnp.mean(center * center, -1, keepdims=True)
    normed = center * lax.rsqrt(spread + 1e-06) * (1.0 + scale_ref[...]) + shift_ref[...]
    values = lax.dot_general(
        normed.astype(jnp.bfloat16),
        head_w[...],
        (((1,), (1,)), ((), ())),
        preferred_element_type=jnp.float32,
    )
    values = (values + bias_ref[...]).astype(jnp.bfloat16)
    features = values.shape[-1]
    patch[...] = jnp.zeros_like(patch)
    patch[:, :features] = values

    moves = [(0, 1), (0, -1), (1, 0), (1, 1), (1, -1)]

    def edge(index, sign):
        dh, ds = moves[index]
        return (
            (h + sign * dh >= 0) & (h + sign * dh < p.nh)
            & (s + sign * ds >= 0) & (s + sign * ds < p.ns)
        )

    def hop(index):
        dh, ds = moves[index]
        return pltpu.make_async_remote_copy(
            src_ref=patch,
            dst_ref=halo.at[index],
            send_sem=s7.at[index],
            recv_sem=r7.at[index],
            device_id={"seq": lax.rem(s + ds + p.ns, p.ns), "head": lax.rem(h + dh, p.nh)},
            device_id_type=MESH,
        )

    for index in range(len(moves)):

        @pl.when(edge(index, 1))
        def _():
            hop(index).start()

    near_ref[1, 1] = values
    for index, (dh, ds) in enumerate(moves):

        @pl.when(edge(index, -1))
        def _():
            hop(index).wait_recv()
            near_ref[1 - dh, 1 - ds] = halo[index][:, :features]

        @pl.when(jnp.logical_not(edge(index, -1)))
        def _():
            near_ref[1 - dh, 1 - ds] = jnp.zeros_like(values)

    for index in range(len(moves)):

        @pl.when(edge(index, 1))
        def _():
            hop(index).wait_send()

    for k in range(2):
        for index, (ds, dh) in enumerate(offsets):
            to_s, copy = sending(index, k)
            guarded(k, ds, s, to_s, copy.wait_send)
    for ds in range(1, p.ns):
        level = lax.rem(s - ds + p.ns, p.ns)

        @pl.when(handed(level))
        def _():
            hand_on(level, place(s, 0), place(peer_s, 0)).wait_send()

    for distance in range(p.ns):
        for i in range(p.units):

            @pl.when((s - distance >= 0) & up_open)
            def _():
                gather_hop(s - distance, i, 1).wait_send()

            @pl.when((s + distance < p.ns) & down_open)
            def _():
                gather_hop(s + distance, i, -1).wait_send()

    for c in range(p.chunks):
        for b in range(p.bits):
            halving(c, b).wait_send()
        for ds in range(1, p.ns):
            to_owner(c, ds, s).wait_send()


def on_device(
    queries,
    attn_keys,
    attn_values,
    residual,
    out_weight,
    out_gate,
    head_shift,
    head_scale,
    head_weight,
    head_bias,
    conv_weight,
    conv_bias,
    norm_gain,
):
    ns, nh = lax.axis_size("seq"), lax.axis_size("head")
    p = Plan(ns, nh, queries, residual, out_weight)
    if not p.fits(queries):
        return on_device_gathered(
            queries, attn_keys, attn_values, residual, out_weight, out_gate, head_shift,
            head_scale, head_weight, head_bias, conv_weight, conv_bias, norm_gain,
        )
    frames, height, breadth, inner = queries.shape
    t, width, patch_size = p.tokens, p.width, head_weight.shape[1]
    dma, bf16 = pltpu.SemaphoreType.DMA, jnp.bfloat16
    tail = (t, p.chunk)
    lanes = -(-patch_size // 128) * 128
    any_spec = pl.BlockSpec(memory_space=pl.ANY)
    vmem = pl.BlockSpec(memory_space=pltpu.VMEM)
    landed = [
        pltpu.VMEM((p.chunks, ns) + ((nh >> 1,) if b == 0 and nh > 2 else ()) + tail, bf16)
        for b in range(p.bits)
    ]
    hidden, near = pl.pallas_call(
        functools.partial(block_kernel, p),
        out_shape=(
            jax.ShapeDtypeStruct((t, width), bf16),
            jax.ShapeDtypeStruct((2, 3, t, patch_size), bf16),
        ),
        in_specs=[any_spec] * 6 + [vmem] * 4,
        out_specs=(vmem, vmem),
        scratch_shapes=[
            pltpu.VMEM((3, t, inner), bf16),
            pltpu.VMEM((2, ns, nh >> 1, 2, 3, t, HEAD_DIM), bf16),
            pltpu.VMEM((ns, p.units, p.slots // p.parts * t, HEAD_DIM), bf16),
            pltpu.VMEM(out_weight.shape, bf16),
            pltpu.VMEM((t, width), bf16),
            pltpu.VMEM(head_weight.shape[::-1], bf16),
            pltpu.VMEM((p.chunks, 2, ns, nh >> 1) + tail, bf16),
            *landed,
            pltpu.VMEM((p.chunks, ns) + tail, bf16),
            pltpu.VMEM((t, lanes), bf16),
            pltpu.VMEM((5, t, lanes), bf16),
            dma((6,)),
            dma((2,)),
            dma((p.slots - 1, 2)),
            dma((p.slots - 1, 2)),
            dma((ns,)),
            dma((ns,)),
            dma((2, ns, p.units)),
            dma((ns, p.units)),
            dma((p.bits, p.chunks)),
            dma((p.bits, p.chunks)),
            dma((ns - 1, p.chunks)),
            dma((ns - 1, p.chunks)),
            dma((5,)),
            dma((5,)),
        ],
        compiler_params=pltpu.CompilerParams(
            collective_id=0, has_side_effects=True, vmem_limit_bytes=60 * 1024 * 1024
        ),
    )(
        queries.reshape(t, inner),
        attn_keys.reshape(t, inner),
        attn_values.reshape(t, inner),
        residual.reshape(t, width),
        out_weight,
        head_weight.T,
        out_gate.reshape(1, -1),
        head_shift.reshape(1, -1),
        head_scale.reshape(1, -1),
        head_bias.reshape(1, -1),
    )
    channels = patch_size // 4
    video = near.reshape(2, 3, frames, height, breadth, 2, 2, channels)
    video = video.transpose(0, 2, 1, 3, 5, 4, 6, 7)
    video = video.reshape(2, frames, 3 * height * 2, breadth * 2, channels)
    video = jnp.concatenate([video[0, -2:], video[1]], 0)
    rows = height * 2
    video = video[:, rows - 1 : 2 * rows + 1]
    padded = jnp.pad(video, ((0, 0), (0, 0), (1, 1), (0, 0)))
    features = convolve(padded, frames, conv_weight, conv_bias, norm_gain)
    return (hidden.reshape(residual.shape), features)


def solution(mesh):
    return jax.shard_map(
        on_device,
        mesh=mesh,
        in_specs=(
            P(("clip", "head"), "seq", None, None),
            P(("clip", "head"), "seq", None, None),
            P(("clip", "head"), "seq", None, None),
            P(("clip", "head"), "seq", None, None),
            P("head", "seq"),
            P(),
            P(),
            P(),
            P(),
            P(),
            P(),
            P(),
            P(),
        ),
        out_specs=(P(("clip", "head"), "seq", None, None), P(("clip", "head"), "seq", None, None)),
        check_vma=False,
    )
```
